256 devices in a mesh: grp: 32 (over z, y_hi, core), seq: 8 (over y_lo, x).
Axes of the slice: x: 4, y: 4 (y_hi: 2, y_lo: 2; y = y_hi * 2 + y_lo), z: 8, core: 2. Of those that a mesh axis runs over, the one named last changes fastest.
Arguments:
- queries: bfloat16 [65536, 4096], P(('grp', 'seq')), may hold values from -8 to 8
- keys: bfloat16 [65536, 4096], P(('grp', 'seq')), may hold values from -6 to 6
- values: bfloat16 [65536, 4096], P(('grp', 'seq')), may hold values from -6 to 6
- global_pos: int32 [512], P(('grp', 'seq')), may hold values from 0 to 127
- layout: int32 [512, 32], P(('grp', 'seq')), may hold values from 0 to 511, all different within a row
Outputs:
- attended: bfloat16 [65536, 4096], P(('grp', 'seq'))
The draws below stay inside these ranges and needn't reach their ends.
Inputs may be any that keep to these rules, and one draw needn't show every extreme that they name: `layout`: each row lists 32 different block indices, and every block is listed by some row.
All inputs are finite; a program needn't handle non-finite values.
Results may differ from the reference program's by a relative error of at most 0.0042.
Values may be sent and summed in bfloat16 or wider, within the bound.
A program may use at most 128 MiB of HBM per device.

```python
import math
import jax
import jax.numpy as jnp
from jax import lax

HEADS = 32
HEAD_DIM = 128
BLOCK = 128
LINKS = 32
WIDTH = 4096
SEQ = 65536
NBLK = 512


def draw_queries(key, part):
    base = jnp.clip(2.0 * jax.random.normal(jax.random.fold_in(key, 1), (SEQ, HEADS * HEAD_DIM), jnp.float32), -8.0, 8.0)
    return base.astype(jnp.bfloat16)


def draw_keys(key, part):
    base = jnp.clip(jax.random.normal(jax.random.fold_in(key, 2), (SEQ, HEADS * HEAD_DIM), jnp.float32), -6.0, 6.0)
    return base.astype(jnp.bfloat16)


def with_ends(entries, key, smallest, largest):
    longest = entries.shape.index(max(entries.shape))
    spots = []
    for shift in (0, 1):
        where = [jax.random.randint(jax.random.fold_in(key, axis), (), 0, length) for axis, length in enumerate(entries.shape)]
        where[longest] = (where[longest] + shift) % entries.shape[longest]
        spots.append(tuple(where))
    return entries.at[spots[0]].set(smallest).at[spots[1]].set(largest)


def shard_levels(key, extent, pieces, smallest, high):
    def one(dim, shards_of):
        heights = jax.random.uniform(jax.random.fold_in(jax.random.fold_in(key, 6), dim), (shards_of,), jnp.float32, smallest / len(pieces), high / len(pieces))
        return jnp.repeat(jnp.exp(heights), extent[dim] // shards_of).reshape((-1,) + (1,) * (len(extent) - dim - 1))

    factor_of = one(*pieces[0])
    for cut in pieces[1:]:
        factor_of = factor_of * one(*cut)
    return factor_of


def picks_of(key, rows, amount, top, lift):
    sequence = jax.random.permutation(jax.random.fold_in(key, 1), amount)
    boost = sequence
    for power in range(3):
        boost = boost * boost // amount
    boost = boost * lift // amount
    lots = jax.random.randint(jax.random.fold_in(key, 2), (rows, amount), 0, 4096) + boost
    sure = jax.random.permutation(jax.random.fold_in(key, 3), rows)[jnp.arange(amount) % rows]
    lots = jnp.where(jnp.arange(rows)[:, None] == sure[None, :], 1 << 14, lots)
    merit = lots * amount + jnp.arange(amount)
    return lax.top_k(merit.astype(jnp.int32), top)[1].astype(jnp.int32)


def noise(rng, dims, scale, reach, split=(), kind=jnp.bfloat16):
    values = jax.random.normal(rng, dims, jnp.float32) * scale
    if len(split) > 0:
        values = shard_levels(rng, dims, split, -0.22, 0.18) * values
    return jnp.clip(values, min=-reach, max=reach).astype(kind)


def setup_inputs(seed: int = 0) -> dict:
    seeds = jax.random.split(jax.random.key(seed), 6)
    return {
        "queries": draw_queries(jax.random.fold_in(seeds[5], 71), 0),
        "keys": draw_keys(jax.random.fold_in(seeds[5], 71), 0),
        "values": noise(seeds[2], (SEQ, WIDTH), 1.0, 6.0, ((0, 256),)),
        "global_pos": with_ends(jax.random.randint(seeds[3], (NBLK,), 0, BLOCK), jax.random.fold_in(seeds[3], 1), 0, BLOCK - 1).astype(jnp.int32),
        "layout": picks_of(seeds[4], NBLK, NBLK, LINKS, 0),
    }


def pooled(source, blocks_all):
    blocks = source.astype(jnp.float32).reshape(blocks_all, BLOCK, HEADS, HEAD_DIM).mean(axis=1)
    spread = lax.optimization_barrier(jnp.mean(blocks * blocks, axis=-1, keepdims=True))
    return (blocks / jnp.sqrt(spread + 1e-06)).reshape(blocks_all, HEADS * HEAD_DIM).astype(jnp.bfloat16)

def reference(queries, keys, values, global_pos, layout):
    score_scale = 1.0 / math.sqrt(HEAD_DIM)
    summary_keys = pooled(keys, NBLK).astype(jnp.float32).reshape(NBLK, HEADS, HEAD_DIM)
    summary_values = pooled(values, NBLK).astype(jnp.float32).reshape(NBLK, HEADS, HEAD_DIM)
    padding = jnp.zeros((BLOCK, HEADS * HEAD_DIM), jnp.bfloat16)
    padded_keys = jnp.concatenate([padding, keys, padding], axis=0)
    padded_values = jnp.concatenate([padding, values, padding], axis=0)
    block_ids = jnp.arange(NBLK, dtype=jnp.int32)

    def one_block(which):
        first_row = (which * BLOCK).astype(jnp.int32)
        query_rows = lax.dynamic_slice_in_dim(queries, first_row, BLOCK, 0).astype(jnp.float32).reshape(BLOCK, HEADS, HEAD_DIM)
        window_keys = lax.dynamic_slice_in_dim(padded_keys, first_row, 3 * BLOCK, 0).astype(jnp.float32).reshape(3 * BLOCK, HEADS, HEAD_DIM)
        window_values = lax.dynamic_slice_in_dim(padded_values, first_row, 3 * BLOCK, 0).astype(jnp.float32).reshape(3 * BLOCK, HEADS, HEAD_DIM)
        window_scores = jnp.einsum('qhd,khd->hqk', query_rows, window_keys) * score_scale
        key_block = jnp.arange(3 * BLOCK, dtype=jnp.int32) // BLOCK + which - 1
        inside = (key_block >= 0) & (key_block < NBLK)
        window_scores = jnp.where(inside[None, None, :], window_scores, -jnp.inf)
        summary_scores = jnp.einsum('qhd,jhd->hqj', query_rows, summary_keys) * score_scale
        listed = jnp.any(layout[which][:, None] == block_ids[None, :], axis=0)
        is_global = jnp.arange(BLOCK, dtype=jnp.int32) == global_pos[which]
        visible = listed[None, :] | is_global[:, None]
        summary_scores = jnp.where(visible[None, :, :], summary_scores, -jnp.inf)
        peak = jnp.maximum(lax.optimization_barrier(jnp.max(window_scores, axis=-1)), lax.optimization_barrier(jnp.max(summary_scores, axis=-1)))
        window_weights = jnp.exp(window_scores - peak[..., None])
        summary_weights = jnp.exp(summary_scores - peak[..., None])
        denominator = lax.optimization_barrier(jnp.sum(window_weights, axis=-1)) + lax.optimization_barrier(jnp.sum(summary_weights, axis=-1))
        rounded_window = lax.optimization_barrier(window_weights.astype(jnp.bfloat16)).astype(jnp.float32)
        rounded_summary = lax.optimization_barrier(summary_weights.astype(jnp.bfloat16)).astype(jnp.float32)
        numerator = jnp.einsum('hqk,khd->hqd', rounded_window, window_values)
        numerator = numerator + jnp.einsum('hqj,jhd->hqd', rounded_summary, summary_values)
        result = numerator / denominator[..., None]
        return jnp.transpose(result, (1, 0, 2)).reshape(BLOCK, HEADS * HEAD_DIM).astype(jnp.bfloat16)
    outputs = lax.map(one_block, block_ids)
    return outputs.reshape(SEQ, HEADS * HEAD_DIM)
```

```python
import math

import jax
import jax.numpy as jnp
from jax import lax
from jax.experimental import pallas as pl
from jax.experimental.pallas import tpu as pltpu
from jax.sharding import PartitionSpec as P

HEADS = 32
HEAD_DIM = 128
BLOCK = 128
WIDTH = HEADS * HEAD_DIM
GROUPS = 32
SEQS = 8
ROWS = 2 * BLOCK
NBLK = 512
CHUNKS = 8
CHUNK_HEADS = HEADS // CHUNKS
CHUNK_WIDTH = WIDTH // CHUNKS
EARLY = 1
EXP_SCALE = math.log2(math.e) / math.sqrt(HEAD_DIM)
MESH = pl.DeviceIdType.MESH
NEG = float("-inf")


def kernel(
    gpos_ref, layout_ref, q_hbm, k_hbm, v_hbm, out_hbm,
    q_ref, k_ref, v_ref, lk_ref, lv_ref, rk_ref, rv_ref, first_ref, sk_ref, sv_ref, out_ref, bias_ref,
    load_sem, halo_send, halo_recv, first_send, first_recv, kz_send, kz_recv, vz_send, vz_recv,
    ky_send, ky_recv, vy_send, vy_recv, core_send, core_recv, out_sem,
):
    grp = lax.axis_index("grp")
    seq = lax.axis_index("seq")
    place = grp * SEQS + seq
    after = lax.rem(place + 1, GROUPS * SEQS)
    before = lax.rem(place + GROUPS * SEQS - 1, GROUPS * SEQS)
    z, y_hi, core = grp // 4, lax.rem(grp // 2, 2), lax.rem(grp, 2)
    y_lo, x = seq // 4, lax.rem(seq, 4)

    def group_at(dz, other_y=False, other_core=False):
        zz = lax.rem(z + dz + 8, 8)
        yy = 1 - y_hi if other_y else y_hi
        cc = 1 - core if other_core else core
        return (zz * 2 + yy) * 2 + cc

    right = (after // SEQS, lax.rem(after, SEQS))
    left = (before // SEQS, lax.rem(before, SEQS))
    x_peers = [(grp, y_lo * 4 + lax.rem(x + d, 4)) for d in (1, 3, 2)]
    y_peer = (grp, (1 - y_lo) * 4 + x)
    y_far = (group_at(0, other_y=True), (1 - y_lo) * 4 + x)
    z_up = (group_at(1), seq)
    z_down = (group_at(-1), seq)
    twin = (group_at(0, other_core=True), seq)

    barrier = pltpu.get_barrier_semaphore()
    partners = [left, right, *x_peers, y_peer, y_far, z_up, z_down, twin]
    for device in partners:
        pl.semaphore_signal(barrier, inc=1, device_id=device, device_id_type=MESH)

    loads = [
        pltpu.make_async_copy(src, dst, load_sem.at[n])
        for n, (src, dst) in enumerate(((k_hbm, k_ref), (v_hbm, v_ref), (q_hbm, q_ref)))
    ]
    for load in loads:
        load.start()
    pl.semaphore_wait(barrier, len(partners))

    def remote(src, dst, send, recv, device):
        return pltpu.make_async_remote_copy(
            src_ref=src, dst_ref=dst, send_sem=send, recv_sem=recv, device_id=device, device_id_type=MESH
        )

    last_rows, first_rows = pl.ds(BLOCK, BLOCK), pl.ds(0, BLOCK)

    def halo(c):
        lanes = pl.ds(pl.multiple_of(c * CHUNK_WIDTH, CHUNK_WIDTH), CHUNK_WIDTH)
        return [
            remote(k_hbm.at[last_rows, lanes], lk_ref.at[:, lanes], halo_send.at[0, c], halo_recv.at[0, c], right),
            remote(k_hbm.at[first_rows, lanes], rk_ref.at[:, lanes], halo_send.at[1, c], halo_recv.at[1, c], left),
            remote(v_hbm.at[last_rows, lanes], lv_ref.at[:, lanes], halo_send.at[2, c], halo_recv.at[2, c], right),
            remote(v_hbm.at[first_rows, lanes], rv_ref.at[:, lanes], halo_send.at[3, c], halo_recv.at[3, c], left),
        ]

    for c in range(EARLY):
        for copy in halo(c):
            copy.start()

    loads[0].wait()
    loads[1].wait()
    for h in range(HEADS):
        lanes = slice(h * HEAD_DIM, (h + 1) * HEAD_DIM)
        means = [
            jnp.sum(ref[b * BLOCK : (b + 1) * BLOCK, lanes].astype(jnp.float32), axis=0, keepdims=True)
            for ref in (k_ref, v_ref)
            for b in range(2)
        ]
        mean = jnp.concatenate(means, axis=0) * (1.0 / BLOCK)
        spread = jnp.mean(mean * mean, axis=-1, keepdims=True)
        first_ref[seq, :, lanes] = (mean / jnp.sqrt(spread + 1e-06)).astype(jnp.bfloat16)

    started = []

    def go(copy):
        copy.start()
        started.append(copy)
        return copy

    x_copies = [
        go(remote(first_ref.at[seq], first_ref.at[seq], first_send.at[n], first_recv.at[n], device))
        for n, device in enumerate(x_peers)
    ]
    for c in range(EARLY, CHUNKS):
        for copy in halo(c):
            copy.start()

    ids = lax.broadcasted_iota(jnp.int32, (1, NBLK), 1)
    rows = lax.broadcasted_iota(jnp.int32, (BLOCK, 1), 0)
    for b in range(2):
        listed = ids == layout_ref[b, 0]
        for n in range(1, layout_ref.shape[1]):
            listed = listed | (ids == layout_ref[b, n])
        bias = jnp.where(listed, 0.0, NEG)
        whole = jnp.where(rows == gpos_ref[b], 0.0, NEG)
        bias_ref[b * BLOCK : (b + 1) * BLOCK, :] = jnp.maximum(bias, whole)

    for copy in x_copies:
        copy.wait_recv()
    quad = pl.ds(y_lo * 4, 4)
    y_copy = go(remote(first_ref.at[quad], first_ref.at[quad], first_send.at[3], first_recv.at[3], y_peer))
    y_copy.wait_recv()

    def rows_of(group):
        return pl.ds(pl.multiple_of(group * 16, 16), 16)

    mine = rows_of(grp)
    for at, ref in ((0, sk_ref), (2, sv_ref)):
        pieces = [first_ref[d, at : at + 2, :].astype(jnp.float32) for d in range(SEQS)]
        ref[mine, :] = jnp.concatenate(pieces, axis=0).astype(jnp.bfloat16)

    def piece(ref, group, send, recv, device):
        return go(remote(ref.at[rows_of(group)], ref.at[rows_of(group)], send, recv, device))

    def arrived(ref, recv):
        pltpu.make_async_copy(ref.at[mine], ref.at[mine], recv).wait()

    cores = [0]

    def to_twin(ref, group, which):
        piece(ref, group, core_send.at[cores[0]], core_recv.at[which], twin)
        cores[0] += 1

    piece(sk_ref, grp, ky_send, ky_recv, y_far)
    piece(sv_ref, grp, vy_send.at[0], vy_recv.at[0], y_far)
    piece(sv_ref, grp, vz_send.at[0, 0], vz_recv.at[0, 0], z_up)
    piece(sv_ref, grp, vz_send.at[1, 0], vz_recv.at[1, 0], z_down)
    piece(sk_ref, grp, kz_send.at[0, 0], kz_recv.at[0, 0], z_up)
    piece(sk_ref, grp, kz_send.at[1, 0], kz_recv.at[1, 0], z_down)
    to_twin(sk_ref, grp, 0)
    to_twin(sv_ref, grp, 1)
    arrived(sk_ref, ky_recv)
    far = group_at(0, other_y=True)
    piece(sk_ref, far, kz_send.at[2, 0], kz_recv.at[2, 0], z_up)
    piece(sk_ref, far, kz_send.at[3, 0], kz_recv.at[3, 0], z_down)
    to_twin(sk_ref, far, 0)
    crossed = [(0, far)]
    for s in range(1, 5):
        for kind, (ref, send, recv, row, dz, steps) in enumerate((
            (sv_ref, vz_send, vz_recv, 0, -s, 4),
            (sv_ref, vz_send, vz_recv, 1, s, 3),
            (sk_ref, kz_send, kz_recv, 0, -s, 4),
            (sk_ref, kz_send, kz_recv, 1, s, 3),
            (sk_ref, kz_send, kz_recv, 2, -s, 3),
            (sk_ref, kz_send, kz_recv, 3, s, 4),
        )):
            if s > steps:
                continue
            group = group_at(dz, other_y=kind >= 4)
            arrived(ref, recv.at[row, s - 1])
            if s < steps:
                piece(ref, group, send.at[row, s], recv.at[row, s], z_up if row % 2 == 0 else z_down)
            if ref is sv_ref:
                n = 2 * s - 1 + row
                piece(ref, group, vy_send.at[n], vy_recv.at[n], y_far)
                crossed.append((n, group_at(dz, other_y=True)))
            to_twin(ref, group, 0 if ref is sk_ref else 1)
        while crossed and (crossed[0][0] < 2 * s - 1 or s == 4):
            n, group = crossed.pop(0)
            arrived(sv_ref, vy_recv.at[n])
            to_twin(sv_ref, group, 1)
    for which, ref in ((0, sk_ref), (1, sv_ref)):
        half = ref.at[pl.ds(0, NBLK // 2)]
        pltpu.make_async_copy(half, half, core_recv.at[which]).wait()

    loads[2].wait()
    bias_left = jnp.where(place == 0, NEG, 0.0)
    bias_right = jnp.where(place == GROUPS * SEQS - 1, NEG, 0.0)
    to_rows = (((1,), (1,)), ((), ()))
    to_cols = (((1,), (0,)), ((), ()))

    def dot(a, b, dims):
        return lax.dot_general(a, b, dims, preferred_element_type=jnp.float32)

    def chunk(c, carry):
        for copy in halo(c):
            copy.wait_recv()
        for n in range(CHUNK_HEADS):
            lanes = pl.ds(pl.multiple_of(c * CHUNK_WIDTH + n * HEAD_DIM, HEAD_DIM), HEAD_DIM)
            q = q_ref[:, lanes]
            s_near = dot(q, k_ref[:, lanes], to_rows)
            s_left = dot(q[:BLOCK], lk_ref[:, lanes], to_rows) + bias_left
            s_right = dot(q[BLOCK:], rk_ref[:, lanes], to_rows) + bias_right
            s_side = jnp.concatenate([s_left, s_right], axis=0)
            s_sum = dot(q, sk_ref[:, lanes], to_rows) + bias_ref[...]
            scores = jnp.concatenate([s_near, s_side, s_sum], axis=1)
            peak = jnp.max(scores, axis=1, keepdims=True)
            weights = jnp.exp2((scores - peak) * EXP_SCALE)
            total = jnp.sum(weights, axis=1, keepdims=True)
            rounded = weights.astype(jnp.bfloat16)
            acc = dot(rounded[:, :ROWS], v_ref[:, lanes], to_cols)
            side = rounded[:, ROWS : ROWS + BLOCK]
            acc += jnp.concatenate([
                dot(side[:BLOCK], lv_ref[:, lanes], to_cols),
                dot(side[BLOCK:], rv_ref[:, lanes], to_cols),
            ], axis=0)
            acc += dot(rounded[:, ROWS + BLOCK :], sv_ref[:, lanes], to_cols)
            out_ref[:, lanes] = (acc / total).astype(jnp.bfloat16)
        store(c).start()
        return carry

    def store(c):
        lanes = pl.ds(pl.multiple_of(c * CHUNK_WIDTH, CHUNK_WIDTH), CHUNK_WIDTH)
        return pltpu.make_async_copy(out_ref.at[:, lanes], out_hbm.at[:, lanes], out_sem.at[c])

    lax.fori_loop(0, CHUNKS, chunk, 0)
    for copy in started:
        copy.wait_send()
    for c in range(CHUNKS):
        for copy in halo(c):
            copy.wait_send()
        store(c).wait()


def shards(queries, keys, values, global_pos, layout):
    bf16 = jnp.bfloat16
    any_spec = pl.BlockSpec(memory_space=pl.ANY)
    smem_spec = pl.BlockSpec(memory_space=pltpu.SMEM)
    dma = pltpu.SemaphoreType.DMA
    return pl.pallas_call(
        kernel,
        out_shape=jax.ShapeDtypeStruct((ROWS, WIDTH), bf16),
        in_specs=[smem_spec, smem_spec, any_spec, any_spec, any_spec],
        out_specs=any_spec,
        scratch_shapes=[
            *[pltpu.VMEM((ROWS, WIDTH), bf16)] * 3,
            *[pltpu.VMEM((BLOCK, WIDTH), bf16)] * 4,
            pltpu.VMEM((SEQS, 4, WIDTH), bf16),
            *[pltpu.VMEM((NBLK, WIDTH), bf16)] * 2,
            pltpu.VMEM((ROWS, WIDTH), bf16),
            pltpu.VMEM((ROWS, NBLK), jnp.float32),
            dma((3,)), dma((4, CHUNKS)), dma((4, CHUNKS)), dma((4,)), dma((4,)),
            dma((4, 4)), dma((4, 4)), dma((2, 4)), dma((2, 4)),
            dma, dma, dma((8,)), dma((8,)), dma((32,)), dma((2,)), dma((CHUNKS,)),
        ],
        compiler_params=pltpu.CompilerParams(collective_id=0, has_side_effects=True),
    )(global_pos, layout, queries, keys, values)


def solution(mesh):
    rows = P(("grp", "seq"), None)
    in_specs = (rows, rows, rows, P(("grp", "seq")), rows)
    return jax.shard_map(shards, mesh=mesh, in_specs=in_specs, out_specs=rows, check_vma=False)
```

```python
import math

import jax
import jax.numpy as jnp
from jax import lax
from jax.experimental import pallas as pl
from jax.experimental.pallas import tpu as pltpu
from jax.sharding import PartitionSpec as P

HEADS = 32
HEAD_DIM = 128
BLOCK = 128
WIDTH = HEADS * HEAD_DIM
GROUPS = 32
SEQS = 8
ROWS = 2 * BLOCK
NBLK = 512
LINKS = 32
CHUNKS = 8
WINDOWS = (0, 0, 2, 3, 5, 7, 8)
PACE = (2, 4, 6, 8, 8)
CHUNK_HEADS = HEADS // CHUNKS
CHUNK_WIDTH = WIDTH // CHUNKS
EXP_SCALE = math.log2(math.e) / math.sqrt(HEAD_DIM)
MESH = pl.DeviceIdType.MESH
NEG = float("-inf")


def kernel(
    gpos_ref, layout_ref, q_hbm, k_hbm, v_hbm, out_ref,
    q_ref, k_ref, v_ref, lk_ref, lv_ref, rk_ref, rv_ref, first_ref, sk_ref, sv_ref,
    acc_ref, peak_ref, total_ref, near_ref, pick_ref, gk_ref, weight_ref, whole_ref, stat_ref, patch_ref,
    load_sem, halo_send, halo_recv, first_send, first_recv, kz_send, kz_recv, vz_send, vz_recv,
    ky_send, ky_recv, vy_send, vy_recv, core_send, core_recv,
):
    grp = lax.axis_index("grp")
    seq = lax.axis_index("seq")
    place = grp * SEQS + seq
    after = lax.rem(place + 1, GROUPS * SEQS)
    before = lax.rem(place + GROUPS * SEQS - 1, GROUPS * SEQS)
    z, y_hi, core = grp // 4, lax.rem(grp // 2, 2), lax.rem(grp, 2)
    y_lo, x = seq // 4, lax.rem(seq, 4)

    def group_at(dz, other_y=False, other_core=False):
        zz = lax.rem(z + dz + 8, 8)
        yy = 1 - y_hi if other_y else y_hi
        cc = 1 - core if other_core else core
        return (zz * 2 + yy) * 2 + cc

    right = (after // SEQS, lax.rem(after, SEQS))
    left = (before // SEQS, lax.rem(before, SEQS))
    x_peers = [(grp, y_lo * 4 + lax.rem(x + d, 4)) for d in (1, 3, 2)]
    y_peer = (grp, (1 - y_lo) * 4 + x)
    y_far = (group_at(0, other_y=True), (1 - y_lo) * 4 + x)
    z_up = (group_at(1), seq)
    z_down = (group_at(-1), seq)
    twin = (group_at(0, other_core=True), seq)

    barrier = pltpu.get_barrier_semaphore()
    partners = [left, right, *x_peers, y_peer, y_far, z_up, z_down, twin]
    for device in partners:
        pl.semaphore_signal(barrier, inc=1, device_id=device, device_id_type=MESH)

    loads = [
        pltpu.make_async_copy(src, dst, load_sem.at[n])
        for n, (src, dst) in enumerate(((k_hbm, k_ref), (v_hbm, v_ref), (q_hbm, q_ref)))
    ]
    for load in loads:
        load.start()
    pl.semaphore_wait(barrier, len(partners))

    def remote(src, dst, send, recv, device):
        return pltpu.make_async_remote_copy(
            src_ref=src, dst_ref=dst, send_sem=send, recv_sem=recv, device_id=device, device_id_type=MESH
        )

    last_rows, first_rows = pl.ds(BLOCK, BLOCK), pl.ds(0, BLOCK)

    def halo(c, side):
        lanes = pl.ds(pl.multiple_of(c * CHUNK_WIDTH, CHUNK_WIDTH), CHUNK_WIDTH)
        rows, device = ((last_rows, right), (first_rows, left))[side]
        return [
            remote(
                src.at[rows, lanes], dst[side].at[:, lanes],
                halo_send.at[2 * n + side, c], halo_recv.at[2 * n + side, c], device,
            )
            for n, (src, dst) in enumerate(((k_hbm, (lk_ref, rk_ref)), (v_hbm, (lv_ref, rv_ref))))
        ]

    turns = (x == 3, x == 0)

    crosses = (turns[0] & (y_lo == 1) & (core == 1), turns[1] & (y_lo == 0) & (core == 0))

    def send_halos(which, first, last):
        for side in range(2):
            @pl.when(which[side])
            def _():
                for c in range(first, last):
                    for copy in halo(c, side)[1 if c == 0 else 0 :]:
                        copy.start()

    for side in range(2):
        halo(0, side)[0].start()

    loads[0].wait()
    loads[1].wait()
    for h in range(HEADS):
        lanes = slice(h * HEAD_DIM, (h + 1) * HEAD_DIM)
        means = [
            jnp.sum(ref[b * BLOCK : (b + 1) * BLOCK, lanes].astype(jnp.float32), axis=0, keepdims=True)
            for ref in (k_ref, v_ref)
            for b in range(2)
        ]
        mean = jnp.concatenate(means, axis=0) * (1.0 / BLOCK)
        spread = jnp.mean(mean * mean, axis=-1, keepdims=True)
        first_ref[seq, :, lanes] = (mean / jnp.sqrt(spread + 1e-06)).astype(jnp.bfloat16)

    started = []

    def go(copy):
        copy.start()
        started.append(copy)
        return copy

    halves = [pl.ds(y_lo * 4 + x, 1), pl.ds((1 - y_lo) * 4 + x, 1)]
    y_copy = go(remote(first_ref.at[halves[0]], first_ref.at[halves[0]], first_send.at[6], first_recv.at[6], y_peer))
    send_halos([~turn for turn in turns], 0, 1)
    x_copies = [
        go(remote(first_ref.at[halves[0]], first_ref.at[halves[0]], first_send.at[n], first_recv.at[n], device))
        for n, device in enumerate(x_peers)
    ]
    y_copy.wait_recv()
    x_copies += [
        go(remote(first_ref.at[halves[1]], first_ref.at[halves[1]], first_send.at[3 + n], first_recv.at[3 + n], device))
        for n, device in enumerate(x_peers)
    ]
    send_halos([~turn for turn in turns], 1, CHUNKS)
    send_halos([turn & ~cross for turn, cross in zip(turns, crosses)], 0, CHUNKS)
    send_halos(crosses, 0, PACE[0])

    lines = lax.broadcasted_iota(jnp.int32, (2 * LINKS, 1), 0)
    index = jnp.zeros((2 * LINKS, 1), jnp.int32)
    for r in range(2 * LINKS):
        index = jnp.where(lines == r, layout_ref[r // LINKS, r % LINKS], index)
    ids = lax.broadcasted_iota(jnp.int32, (2 * LINKS, NBLK), 1)
    pick_ref[...] = jnp.where(ids == index, 1.0, 0.0).astype(jnp.bfloat16)

    loads[2].wait()
    bias_left = jnp.where(place == 0, NEG, 0.0)
    bias_right = jnp.where(place == GROUPS * SEQS - 1, NEG, 0.0)
    to_rows = (((1,), (1,)), ((), ()))
    to_cols = (((1,), (0,)), ((), ()))

    def dot(a, b, dims):
        return lax.dot_general(a, b, dims, preferred_element_type=jnp.float32)

    def chunk_lanes(c):
        return pl.ds(pl.multiple_of(c * CHUNK_WIDTH, CHUNK_WIDTH), CHUNK_WIDTH)

    def head_lanes(c, n):
        return pl.ds(pl.multiple_of(c * CHUNK_WIDTH + n * HEAD_DIM, HEAD_DIM), HEAD_DIM)

    def spread_out(column):
        return jnp.broadcast_to(column, (column.shape[0], HEAD_DIM))

    def window(c, carry):
        for copy in halo(c, 0) + halo(c, 1):
            copy.wait_recv()
        for n in range(CHUNK_HEADS):
            lanes = head_lanes(c, n)
            q = q_ref[:, lanes]
            s_near = dot(q, k_ref[:, lanes], to_rows)
            s_left = dot(q[:BLOCK], lk_ref[:, lanes], to_rows) + bias_left
            s_right = dot(q[BLOCK:], rk_ref[:, lanes], to_rows) + bias_right
            scores = jnp.concatenate([s_near, jnp.concatenate([s_left, s_right], axis=0)], axis=1)
            peak = jnp.max(scores, axis=1, keepdims=True)
            weights = jnp.exp2((scores - peak) * EXP_SCALE)
            rounded = weights.astype(jnp.bfloat16)
            side = rounded[:, ROWS:]
            acc_ref[:, lanes] = dot(rounded[:, :ROWS], v_ref[:, lanes], to_cols) + jnp.concatenate([
                dot(side[:BLOCK], lv_ref[:, lanes], to_cols),
                dot(side[BLOCK:], rv_ref[:, lanes], to_cols),
            ], axis=0)
            peak_ref[:, lanes] = spread_out(peak)
            total_ref[:, lanes] = spread_out(jnp.sum(weights, axis=1, keepdims=True))
        return carry

    def windows(n):
        first, last = WINDOWS[n : n + 2]
        if first < last:
            lax.fori_loop(first, last, window, 0)

    head_of_row = lax.rem(lax.broadcasted_iota(jnp.int32, (2 * HEADS, CHUNK_WIDTH), 0), HEADS)
    head_of_lane = lax.broadcasted_iota(jnp.int32, (2 * HEADS, CHUNK_WIDTH), 1) // HEAD_DIM

    def own_head(c):
        return head_of_row == head_of_lane + c * CHUNK_HEADS

    def use_keys(c, carry):
        lanes = chunk_lanes(c)
        keys = sk_ref[:, lanes]
        gk_ref[:, lanes] = dot(pick_ref[...], keys, to_cols).astype(jnp.bfloat16)
        whole = dot(choose, q_ref[:, lanes], to_cols)
        rows = jnp.concatenate([jnp.broadcast_to(whole[b : b + 1], (HEADS, CHUNK_WIDTH)) for b in range(2)], axis=0)
        rows = jnp.where(own_head(c), rows, 0.0).astype(jnp.bfloat16)
        old = jnp.where(c == 0, 0.0, whole_ref[...])
        whole_ref[...] = old + dot(rows, keys, to_rows)
        return carry

    choose_row = lax.broadcasted_iota(jnp.int32, (8, ROWS), 0)
    choose_col = lax.broadcasted_iota(jnp.int32, (8, ROWS), 1)
    choose = jnp.zeros((8, ROWS), jnp.float32)
    for b in range(2):
        choose = jnp.where((choose_row == b) & (choose_col == b * BLOCK + gpos_ref[b]), 1.0, choose)
    choose = choose.astype(jnp.bfloat16)

    def whole_weights():
        scores = whole_ref[...]
        peak = jnp.max(scores, axis=1, keepdims=True)
        weights = jnp.exp2((scores - peak) * EXP_SCALE)
        stat_ref[0] = spread_out(peak)
        stat_ref[1] = spread_out(jnp.sum(weights, axis=1, keepdims=True))
        whole_ref[...] = weights

    def own_sum(own, value, b):
        rows = slice(b * HEADS, (b + 1) * HEADS)
        return jnp.sum(jnp.where(own[rows], value[rows], 0.0), axis=0, keepdims=True)

    row_ids = lax.broadcasted_iota(jnp.int32, (ROWS, HEAD_DIM), 0)
    whole_row = (row_ids == gpos_ref[0]) | (row_ids == BLOCK + gpos_ref[1])
    link_rows = lax.broadcasted_iota(jnp.int32, (ROWS, 2 * LINKS), 0) // BLOCK
    link_cols = lax.broadcasted_iota(jnp.int32, (ROWS, 2 * LINKS), 1) // LINKS

    def listed(c, carry):
        for n in range(CHUNK_HEADS):
            lanes = head_lanes(c, n)
            scores = dot(q_ref[:, lanes], gk_ref[:, lanes], to_rows)
            scores = jnp.where(link_rows == link_cols, scores, NEG)
            here = peak_ref[:, lanes]
            peak = jnp.maximum(here, spread_out(jnp.max(scores, axis=1, keepdims=True)))
            keep = jnp.exp2((here - peak) * EXP_SCALE)
            weights = jnp.exp2((scores - peak[:, : 2 * LINKS]) * EXP_SCALE)
            total = total_ref[:, lanes] * keep + spread_out(jnp.sum(weights, axis=1, keepdims=True))
            share = 1.0 / total
            weight_ref[c * CHUNK_HEADS + n] = (weights * share[:, : 2 * LINKS]).astype(jnp.bfloat16)
            near_ref[:, lanes] = acc_ref[:, lanes] * (keep * share)
        lanes = chunk_lanes(c)
        own = own_head(c)
        tops, sums = (jnp.tile(stat_ref[n], (1, CHUNK_HEADS)) for n in range(2))
        for b in range(2):
            at = pl.ds(b * BLOCK + gpos_ref[b], 1)
            here, top = peak_ref[at, lanes], own_sum(own, tops, b)
            peak = jnp.maximum(here, top)
            keep = jnp.exp2((here - peak) * EXP_SCALE)
            more = jnp.exp2((top - peak) * EXP_SCALE)
            share = 1.0 / (total_ref[at, lanes] * keep + own_sum(own, sums, b) * more)
            patch_ref[2 * b, :, lanes] = jnp.broadcast_to(acc_ref[at, lanes] * (keep * share), (8, CHUNK_WIDTH))
            patch_ref[2 * b + 1, :, lanes] = jnp.broadcast_to(more * share, (8, CHUNK_WIDTH))
        return carry

    def finish(c, carry):
        lanes = chunk_lanes(c)
        vals = sv_ref[:, lanes]
        chosen = dot(pick_ref[...], vals, to_cols).astype(jnp.bfloat16)
        own = own_head(c)
        acc = dot(whole_ref[...].astype(jnp.bfloat16), vals, to_cols)
        patches = [
            patch_ref[2 * b, 0:1, lanes] + own_sum(own, acc, b) * patch_ref[2 * b + 1, 0:1, lanes] for b in range(2)
        ]
        for n in range(CHUNK_HEADS):
            lanes = head_lanes(c, n)
            part = slice(n * HEAD_DIM, (n + 1) * HEAD_DIM)
            result = near_ref[:, lanes] + dot(weight_ref[c * CHUNK_HEADS + n], chosen[:, part], to_cols)
            patch = jnp.concatenate([jnp.broadcast_to(p[:, part], (BLOCK, HEAD_DIM)) for p in patches], axis=0)
            out_ref[:, lanes] = jnp.where(whole_row, patch, result).astype(jnp.bfloat16)
        return carry

    for copy in x_copies:
        copy.wait_recv()
    def rows_of(group):
        return pl.ds(pl.multiple_of(group * 16, 16), 16)

    mine = rows_of(grp)
    for at, ref in ((0, sk_ref), (2, sv_ref)):
        pieces = [first_ref[d, at : at + 2, :].astype(jnp.float32) for d in range(SEQS)]
        ref[mine, :] = jnp.concatenate(pieces, axis=0).astype(jnp.bfloat16)

    def piece(ref, group, send, recv, device):
        remote(ref.at[rows_of(group)], ref.at[rows_of(group)], send, recv, device).start()

    def arrived(ref, recv):
        pltpu.make_async_copy(ref.at[mine], ref.at[mine], recv).wait()

    def to_twin(ref, group, which, slot):
        piece(ref, group, core_send.at[slot], core_recv.at[which], twin)

    busy = ((x == 0) & (y_hi == 0) & (y_lo == 0)) | ((x == 3) & (y_hi == 1) & (y_lo == 1))
    sign = jnp.where(x == 0, 1, -1)
    ahead, behind = (group_at(sign), seq), (group_at(-sign), seq)

    piece(sk_ref, grp, ky_send, ky_recv, y_far)
    piece(sv_ref, grp, vy_send.at[0], vy_recv.at[0], y_far)
    piece(sv_ref, grp, vz_send.at[0, 0], vz_recv.at[0, 0], ahead)
    piece(sv_ref, grp, vz_send.at[1, 0], vz_recv.at[1, 0], behind)
    piece(sk_ref, grp, kz_send.at[0, 0], kz_recv.at[0, 0], ahead)
    piece(sk_ref, grp, kz_send.at[1, 0], kz_recv.at[1, 0], behind)
    to_twin(sk_ref, grp, 1, 8)
    to_twin(sv_ref, grp, 0, 0)
    arrived(sk_ref, ky_recv)
    far = group_at(0, other_y=True)
    piece(sk_ref, far, kz_send.at[2, 0], kz_recv.at[2, 0], ahead)
    piece(sk_ref, far, kz_send.at[3, 0], kz_recv.at[3, 0], behind)
    to_twin(sk_ref, far, 1, 16)
    send_halos(crosses, PACE[0], PACE[1])
    crossed = [(0, far)]
    for s in range(1, 6):
        for kind, (ref, send, recv, row) in enumerate((
            (sv_ref, vz_send, vz_recv, 0), (sk_ref, kz_send, kz_recv, 0), (sk_ref, kz_send, kz_recv, 2),
        )):
            for side in range(2):
                usual, other = ((3, 4), (4, 3))[side] if kind == 2 else ((4, 5), (3, 2))[side]
                fewest, most = min(usual, other), max(usual, other)
                if s > most:
                    continue
                longer = busy if other > usual else ~busy
                dz = (-sign if side == 0 else sign) * s
                group = group_at(dz, other_y=kind == 2)
                n = {4: 7, 5: 6}.get(s, 2 * s - 1 + side)

                def forward():
                    piece(ref, group, send.at[row + side, s], recv.at[row + side, s], (ahead, behind)[side])

                def pass_on():
                    arrived(ref, recv.at[row + side, s - 1])
                    if s < fewest:
                        forward()
                    elif s < most:
                        pl.when(longer)(forward) if s == fewest else forward()
                    if kind == 0:
                        piece(ref, group, vy_send.at[n], vy_recv.at[n], y_far)
                    to_twin(ref, group, min(kind, 1), kind * 8 + n)

                if s <= fewest:
                    pass_on()
                else:
                    pl.when(longer)(pass_on)
                if kind == 0 and s < 5:
                    if (s, side) != (4, 1):
                        crossed.append((n, group_at(dz, other_y=True)))
        if s + 1 < len(PACE):
            send_halos(crosses, PACE[s], PACE[s + 1])
        windows(s)
        while crossed and (crossed[0][0] < 2 * s - 1 and crossed[0][0] < 6 or s == 5):
            n, group = crossed.pop(0)
            arrived(sv_ref, vy_recv.at[n])
            to_twin(sv_ref, group, 0, 24 + n)
    for which, ref in ((1, sk_ref), (0, sv_ref)):
        half = ref.at[pl.ds(0, NBLK // 2)]
        pltpu.make_async_copy(half, half, core_recv.at[which]).wait()
        if which == 1:
            lax.fori_loop(0, CHUNKS, use_keys, 0)
            whole_weights()
            lax.fori_loop(0, CHUNKS, listed, 0)
    lax.fori_loop(0, CHUNKS, finish, 0)
    for copy in started:
        copy.wait_send()

    def sent(ref, send):
        pltpu.make_async_copy(ref.at[mine], ref.at[mine], send).wait()

    sent(sk_ref, ky_send)
    for n in range(8):
        sent(sv_ref, vy_send.at[n])
    for n in range(32):
        sent(sv_ref, core_send.at[n])
    for ref, send, row, (usual, other) in (
        (sv_ref, vz_send, 0, (4, 5)), (sv_ref, vz_send, 1, (3, 2)), (sk_ref, kz_send, 0, (4, 5)),
        (sk_ref, kz_send, 1, (3, 2)), (sk_ref, kz_send, 2, (3, 4)), (sk_ref, kz_send, 3, (4, 3)),
    ):
        for n in range(max(usual, other)):
            if n < min(usual, other):
                sent(ref, send.at[row, n])
            else:
                pl.when(busy if other > usual else ~busy)(lambda: sent(ref, send.at[row, n]))
    for c in range(CHUNKS):
        for copy in halo(c, 0) + halo(c, 1):
            copy.wait_send()


def shards(queries, keys, values, global_pos, layout):
    bf16 = jnp.bfloat16
    hbm_spec = pl.BlockSpec(memory_space=pltpu.HBM)
    smem_spec = pl.BlockSpec(memory_space=pltpu.SMEM)
    dma = pltpu.SemaphoreType.DMA
    return pl.pallas_call(
        kernel,
        out_shape=jax.ShapeDtypeStruct((ROWS, WIDTH), bf16),
        in_specs=[smem_spec, smem_spec, hbm_spec, hbm_spec, hbm_spec],
        out_specs=pl.BlockSpec(memory_space=pltpu.VMEM),
        scratch_shapes=[
            *[pltpu.VMEM((ROWS, WIDTH), bf16)] * 3,
            *[pltpu.VMEM((BLOCK, WIDTH), bf16)] * 4,
            pltpu.VMEM((SEQS, 4, WIDTH), bf16),
            *[pltpu.VMEM((NBLK, WIDTH), bf16)] * 2,
            *[pltpu.VMEM((ROWS, WIDTH), jnp.float32)] * 4,
            pltpu.VMEM((2 * LINKS, NBLK), bf16),
            pltpu.VMEM((2 * LINKS, WIDTH), bf16),
            pltpu.VMEM((HEADS, ROWS, 2 * LINKS), bf16),
            pltpu.VMEM((2 * HEADS, NBLK), jnp.float32),
            pltpu.VMEM((2, 2 * HEADS, HEAD_DIM), jnp.float32),
            pltpu.VMEM((4, 8, WIDTH), jnp.float32),
            dma((3,)), dma((4, CHUNKS)), dma((4, CHUNKS)), dma((7,)), dma((7,)),
            dma((4, 5)), dma((4, 5)), dma((2, 5)), dma((2, 5)),
            dma, dma, dma((8,)), dma((8,)), dma((32,)), dma((2,)),
        ],
        compiler_params=pltpu.CompilerParams(collective_id=0, has_side_effects=True, vmem_limit_bytes=50 * 1024 * 1024),
    )(global_pos, layout, queries, keys, values)


def solution(mesh):
    rows = P(("grp", "seq"), None)
    in_specs = (rows, rows, rows, P(("grp", "seq")), rows)
    return jax.shard_map(shards, mesh=mesh, in_specs=in_specs, out_specs=rows, check_vma=False)
```

```python
import math

import jax
import jax.numpy as jnp
from jax import lax
from jax.experimental import pallas as pl
from jax.experimental.pallas import tpu as pltpu
from jax.sharding import PartitionSpec as P

HEADS = 32
HEAD_DIM = 128
BLOCK = 128
WIDTH = HEADS * HEAD_DIM
GROUPS = 32
SEQS = 8
ROWS = 2 * BLOCK
NBLK = 512
LINKS = 32
CHUNKS = 8
WINDOWS = (0, 0, 2, 3, 5, 7, 8)
PACE = (2, 4, 6, 7, 8)
CHUNK_HEADS = HEADS // CHUNKS
CHUNK_WIDTH = WIDTH // CHUNKS
EXP_SCALE = math.log2(math.e) / math.sqrt(HEAD_DIM)
MESH = pl.DeviceIdType.MESH
NEG = float("-inf")


def kernel(
    gpos_ref, layout_ref, q_hbm, k_hbm, v_hbm, out_ref,
    q_ref, k_ref, v_ref, lk_ref, lv_ref, rk_ref, rv_ref, first_ref, sk_ref, sv_ref,
    acc_ref, peak_ref, total_ref, near_ref, pick_ref, gk_ref, weight_ref, whole_ref, stat_ref, patch_ref,
    load_sem, halo_send, halo_recv, first_send, first_recv, kz_send, kz_recv, vz_send, vz_recv,
    ky_send, ky_recv, vy_send, vy_recv, core_send, core_recv,
):
    grp = lax.axis_index("grp")
    seq = lax.axis_index("seq")
    place = grp * SEQS + seq
    after = lax.rem(place + 1, GROUPS * SEQS)
    before = lax.rem(place + GROUPS * SEQS - 1, GROUPS * SEQS)
    z, y_hi, core = grp // 4, lax.rem(grp // 2, 2), lax.rem(grp, 2)
    y_lo, x = seq // 4, lax.rem(seq, 4)

    def group_at(dz, other_y=False, other_core=False):
        zz = lax.rem(z + dz + 8, 8)
        yy = 1 - y_hi if other_y else y_hi
        cc = 1 - core if other_core else core
        return (zz * 2 + yy) * 2 + cc

    right = (after // SEQS, lax.rem(after, SEQS))
    left = (before // SEQS, lax.rem(before, SEQS))
    x_peers = [(grp, y_lo * 4 + lax.rem(x + d, 4)) for d in (1, 3, 2)]
    y_peer = (grp, (1 - y_lo) * 4 + x)
    y_far = (group_at(0, other_y=True), (1 - y_lo) * 4 + x)
    z_up = (group_at(1), seq)
    z_down = (group_at(-1), seq)
    twin = (group_at(0, other_core=True), seq)

    barrier = pltpu.get_barrier_semaphore()
    partners = [left, right, *x_peers, y_peer, y_far, z_up, z_down, twin]
    for device in partners:
        pl.semaphore_signal(barrier, inc=1, device_id=device, device_id_type=MESH)

    loads = [
        pltpu.make_async_copy(src, dst, load_sem.at[n])
        for n, (src, dst) in enumerate(((k_hbm, k_ref), (v_hbm, v_ref), (q_hbm, q_ref)))
    ]
    for load in loads:
        load.start()
    pl.semaphore_wait(barrier, len(partners))

    def remote(src, dst, send, recv, device):
        return pltpu.make_async_remote_copy(
            src_ref=src, dst_ref=dst, send_sem=send, recv_sem=recv, device_id=device, device_id_type=MESH
        )

    last_rows, first_rows = pl.ds(BLOCK, BLOCK), pl.ds(0, BLOCK)

    def halo(c, side):
        lanes = pl.ds(pl.multiple_of(c * CHUNK_WIDTH, CHUNK_WIDTH), CHUNK_WIDTH)
        rows, device = ((last_rows, right), (first_rows, left))[side]
        return [
            remote(
                src.at[rows, lanes], dst[side].at[:, lanes],
                halo_send.at[2 * n + side, c], halo_recv.at[2 * n + side, c], device,
            )
            for n, (src, dst) in enumerate(((k_hbm, (lk_ref, rk_ref)), (v_hbm, (lv_ref, rv_ref))))
        ]

    turns = (x == 3, x == 0)

    crosses = (turns[0] & (y_lo == 1) & (core == 1), turns[1] & (y_lo == 0) & (core == 0))

    def send_halos(which, first, last):
        for side in range(2):
            @pl.when(which[side])
            def _():
                for c in range(first, last):
                    for copy in halo(c, side)[1 if c == 0 else 0 :]:
                        copy.start()

    for side in range(2):
        halo(0, side)[0].start()

    loads[0].wait()
    loads[1].wait()
    for h in range(HEADS):
        lanes = slice(h * HEAD_DIM, (h + 1) * HEAD_DIM)
        means = [
            jnp.sum(ref[b * BLOCK : (b + 1) * BLOCK, lanes].astype(jnp.float32), axis=0, keepdims=True)
            for ref in (k_ref, v_ref)
            for b in range(2)
        ]
        mean = jnp.concatenate(means, axis=0) * (1.0 / BLOCK)
        spread = jnp.mean(mean * mean, axis=-1, keepdims=True)
        first_ref[seq, :, lanes] = (mean / jnp.sqrt(spread + 1e-06)).astype(jnp.bfloat16)

    started = []

    def go(copy):
        copy.start()
        started.append(copy)
        return copy

    halves = [pl.ds(y_lo * 4 + x, 1), pl.ds((1 - y_lo) * 4 + x, 1)]
    y_copy = go(remote(first_ref.at[halves[0]], first_ref.at[halves[0]], first_send.at[6], first_recv.at[6], y_peer))
    send_halos([~turn for turn in turns], 0, 1)
    x_copies = [
        go(remote(first_ref.at[halves[0]], first_ref.at[halves[0]], first_send.at[n], first_recv.at[n], device))
        for n, device in enumerate(x_peers)
    ]
    y_copy.wait_recv()
    x_copies += [
        go(remote(first_ref.at[halves[1]], first_ref.at[halves[1]], first_send.at[3 + n], first_recv.at[3 + n], device))
        for n, device in enumerate(x_peers)
    ]
    send_halos([~turn for turn in turns], 1, CHUNKS)
    send_halos([turn & ~cross for turn, cross in zip(turns, crosses)], 0, CHUNKS)
    send_halos(crosses, 0, PACE[0])

    lines = lax.broadcasted_iota(jnp.int32, (2 * LINKS, 1), 0)
    index = jnp.zeros((2 * LINKS, 1), jnp.int32)
    for r in range(2 * LINKS):
        index = jnp.where(lines == r, layout_ref[r // LINKS, r % LINKS], index)
    ids = lax.broadcasted_iota(jnp.int32, (2 * LINKS, NBLK), 1)
    pick_ref[...] = jnp.where(ids == index, 1.0, 0.0).astype(jnp.bfloat16)

    loads[2].wait()
    bias_left = jnp.where(place == 0, NEG, 0.0)
    bias_right = jnp.where(place == GROUPS * SEQS - 1, NEG, 0.0)
    to_rows = (((1,), (1,)), ((), ()))
    to_cols = (((1,), (0,)), ((), ()))

    def dot(a, b, dims):
        return lax.dot_general(a, b, dims, preferred_element_type=jnp.float32)

    def chunk_lanes(c):
        return pl.ds(pl.multiple_of(c * CHUNK_WIDTH, CHUNK_WIDTH), CHUNK_WIDTH)

    def head_lanes(c, n):
        return pl.ds(pl.multiple_of(c * CHUNK_WIDTH + n * HEAD_DIM, HEAD_DIM), HEAD_DIM)

    def spread_out(column):
        return jnp.broadcast_to(column, (column.shape[0], HEAD_DIM))

    def window(c, carry):
        for copy in halo(c, 0) + halo(c, 1):
            copy.wait_recv()
        for n in range(CHUNK_HEADS):
            lanes = head_lanes(c, n)
            q = q_ref[:, lanes]
            s_near = dot(q, k_ref[:, lanes], to_rows)
            s_left = dot(q[:BLOCK], lk_ref[:, lanes], to_rows) + bias_left
            s_right = dot(q[BLOCK:], rk_ref[:, lanes], to_rows) + bias_right
            scores = jnp.concatenate([s_near, jnp.concatenate([s_left, s_right], axis=0)], axis=1)
            peak = jnp.max(scores, axis=1, keepdims=True)
            weights = jnp.exp2((scores - peak) * EXP_SCALE)
            rounded = weights.astype(jnp.bfloat16)
            side = rounded[:, ROWS:]
            acc_ref[:, lanes] = dot(rounded[:, :ROWS], v_ref[:, lanes], to_cols) + jnp.concatenate([
                dot(side[:BLOCK], lv_ref[:, lanes], to_cols),
                dot(side[BLOCK:], rv_ref[:, lanes], to_cols),
            ], axis=0)
            peak_ref[:, lanes] = spread_out(peak)
            total_ref[:, lanes] = spread_out(jnp.sum(weights, axis=1, keepdims=True))
        return carry

    def windows(n):
        first, last = WINDOWS[n : n + 2]
        if first < last:
            lax.fori_loop(first, last, window, 0)

    head_of_row = lax.rem(lax.broadcasted_iota(jnp.int32, (2 * HEADS, CHUNK_WIDTH), 0), HEADS)
    head_of_lane = lax.broadcasted_iota(jnp.int32, (2 * HEADS, CHUNK_WIDTH), 1) // HEAD_DIM

    def own_head(c):
        return head_of_row == head_of_lane + c * CHUNK_HEADS

    def use_keys(c, carry):
        lanes = chunk_lanes(c)
        keys = sk_ref[:, lanes]
        gk_ref[:, lanes] = dot(pick_ref[...], keys, to_cols).astype(jnp.bfloat16)
        whole = dot(choose, q_ref[:, lanes], to_cols)
        rows = jnp.concatenate([jnp.broadcast_to(whole[b : b + 1], (HEADS, CHUNK_WIDTH)) for b in range(2)], axis=0)
        rows = jnp.where(own_head(c), rows, 0.0).astype(jnp.bfloat16)
        old = jnp.where(c == 0, 0.0, whole_ref[...])
        whole_ref[...] = old + dot(rows, keys, to_rows)
        return carry

    choose_row = lax.broadcasted_iota(jnp.int32, (8, ROWS), 0)
    choose_col = lax.broadcasted_iota(jnp.int32, (8, ROWS), 1)
    choose = jnp.zeros((8, ROWS), jnp.float32)
    for b in range(2):
        choose = jnp.where((choose_row == b) & (choose_col == b * BLOCK + gpos_ref[b]), 1.0, choose)
    choose = choose.astype(jnp.bfloat16)

    def whole_weights():
        scores = whole_ref[...]
        peak = jnp.max(scores, axis=1, keepdims=True)
        weights = jnp.exp2((scores - peak) * EXP_SCALE)
        stat_ref[0] = spread_out(peak)
        stat_ref[1] = spread_out(jnp.sum(weights, axis=1, keepdims=True))
        whole_ref[...] = weights

    def own_sum(own, value, b):
        rows = slice(b * HEADS, (b + 1) * HEADS)
        return jnp.sum(jnp.where(own[rows], value[rows], 0.0), axis=0, keepdims=True)

    row_ids = lax.broadcasted_iota(jnp.int32, (ROWS, HEAD_DIM), 0)
    whole_row = (row_ids == gpos_ref[0]) | (row_ids == BLOCK + gpos_ref[1])
    link_rows = lax.broadcasted_iota(jnp.int32, (ROWS, 2 * LINKS), 0) // BLOCK
    link_cols = lax.broadcasted_iota(jnp.int32, (ROWS, 2 * LINKS), 1) // LINKS

    def listed(c, carry):
        for n in range(CHUNK_HEADS):
            lanes = head_lanes(c, n)
            scores = dot(q_ref[:, lanes], gk_ref[:, lanes], to_rows)
            scores = jnp.where(link_rows == link_cols, scores, NEG)
            here = peak_ref[:, lanes]
            peak = jnp.maximum(here, spread_out(jnp.max(scores, axis=1, keepdims=True)))
            keep = jnp.exp2((here - peak) * EXP_SCALE)
            weights = jnp.exp2((scores - peak[:, : 2 * LINKS]) * EXP_SCALE)
            total = total_ref[:, lanes] * keep + spread_out(jnp.sum(weights, axis=1, keepdims=True))
            share = 1.0 / total
            weight_ref[c * CHUNK_HEADS + n] = (weights * share[:, : 2 * LINKS]).astype(jnp.bfloat16)
            near_ref[:, lanes] = acc_ref[:, lanes] * (keep * share)
        lanes = chunk_lanes(c)
        own = own_head(c)
        tops, sums = (jnp.tile(stat_ref[n], (1, CHUNK_HEADS)) for n in range(2))
        for b in range(2):
            at = pl.ds(b * BLOCK + gpos_ref[b], 1)
            here, top = peak_ref[at, lanes], own_sum(own, tops, b)
            peak = jnp.maximum(here, top)
            keep = jnp.exp2((here - peak) * EXP_SCALE)
            more = jnp.exp2((top - peak) * EXP_SCALE)
            share = 1.0 / (total_ref[at, lanes] * keep + own_sum(own, sums, b) * more)
            patch_ref[2 * b, :, lanes] = jnp.broadcast_to(acc_ref[at, lanes] * (keep * share), (8, CHUNK_WIDTH))
            patch_ref[2 * b + 1, :, lanes] = jnp.broadcast_to(more * share, (8, CHUNK_WIDTH))
        return carry

    def finish(c, carry):
        lanes = chunk_lanes(c)
        vals = sv_ref[:, lanes]
        chosen = dot(pick_ref[...], vals, to_cols).astype(jnp.bfloat16)
        own = own_head(c)
        acc = dot(whole_ref[...].astype(jnp.bfloat16), vals, to_cols)
        patches = [
            patch_ref[2 * b, 0:1, lanes] + own_sum(own, acc, b) * patch_ref[2 * b + 1, 0:1, lanes] for b in range(2)
        ]
        for n in range(CHUNK_HEADS):
            lanes = head_lanes(c, n)
            part = slice(n * HEAD_DIM, (n + 1) * HEAD_DIM)
            result = near_ref[:, lanes] + dot(weight_ref[c * CHUNK_HEADS + n], chosen[:, part], to_cols)
            patch = jnp.concatenate([jnp.broadcast_to(p[:, part], (BLOCK, HEAD_DIM)) for p in patches], axis=0)
            out_ref[:, lanes] = jnp.where(whole_row, patch, result).astype(jnp.bfloat16)
        return carry

    for copy in x_copies:
        copy.wait_recv()
    def rows_of(group):
        return pl.ds(pl.multiple_of(group * 16, 16), 16)

    mine = rows_of(grp)
    for at, ref in ((0, sk_ref), (2, sv_ref)):
        pieces = [first_ref[d, at : at + 2, :].astype(jnp.float32) for d in range(SEQS)]
        ref[mine, :] = jnp.concatenate(pieces, axis=0).astype(jnp.bfloat16)

    def piece(ref, group, send, recv, device):
        remote(ref.at[rows_of(group)], ref.at[rows_of(group)], send, recv, device).start()

    def arrived(ref, recv):
        pltpu.make_async_copy(ref.at[mine], ref.at[mine], recv).wait()

    def to_twin(ref, group, which, slot):
        piece(ref, group, core_send.at[slot], core_recv.at[which], twin)

    busy = ((x == 0) & (y_hi == 0) & (y_lo == 0)) | ((x == 3) & (y_hi == 1) & (y_lo == 1))
    sign = jnp.where(x == 0, 1, -1)
    ahead, behind = (group_at(sign), seq), (group_at(-sign), seq)

    piece(sk_ref, grp, ky_send, ky_recv, y_far)
    piece(sv_ref, grp, vy_send.at[0], vy_recv.at[0], y_far)
    piece(sv_ref, grp, vz_send.at[0, 0], vz_recv.at[0, 0], ahead)
    piece(sv_ref, grp, vz_send.at[1, 0], vz_recv.at[1, 0], behind)
    piece(sk_ref, grp, kz_send.at[0, 0], kz_recv.at[0, 0], ahead)
    piece(sk_ref, grp, kz_send.at[1, 0], kz_recv.at[1, 0], behind)
    to_twin(sk_ref, grp, 1, 8)
    to_twin(sv_ref, grp, 0, 0)
    arrived(sk_ref, ky_recv)
    far = group_at(0, other_y=True)
    piece(sk_ref, far, kz_send.at[2, 0], kz_recv.at[2, 0], ahead)
    piece(sk_ref, far, kz_send.at[3, 0], kz_recv.at[3, 0], behind)
    to_twin(sk_ref, far, 1, 16)
    send_halos(crosses, PACE[0], PACE[1])
    crossed = [(0, far)]
    for s in range(1, 6):
        for kind, (ref, send, recv, row) in enumerate((
            (sv_ref, vz_send, vz_recv, 0), (sk_ref, kz_send, kz_recv, 0), (sk_ref, kz_send, kz_recv, 2),
        )):
            for side in range(2):
                usual, other = ((3, 4), (4, 3))[side] if kind == 2 else ((4, 5), (3, 2))[side]
                fewest, most = min(usual, other), max(usual, other)
                if s > most:
                    continue
                longer = busy if other > usual else ~busy
                dz = (-sign if side == 0 else sign) * s
                group = group_at(dz, other_y=kind == 2)
                n = {4: 7, 5: 6}.get(s, 2 * s - 1 + side)

                def forward():
                    piece(ref, group, send.at[row + side, s], recv.at[row + side, s], (ahead, behind)[side])

                def pass_on():
                    arrived(ref, recv.at[row + side, s - 1])
                    if s < fewest:
                        forward()
                    elif s < most:
                        pl.when(longer)(forward) if s == fewest else forward()
                    if kind == 0:
                        piece(ref, group, vy_send.at[n], vy_recv.at[n], y_far)
                    to_twin(ref, group, min(kind, 1), kind * 8 + n)

                if s <= fewest:
                    pass_on()
                else:
                    pl.when(longer)(pass_on)
                if kind == 0 and s < 5:
                    if (s, side) != (4, 1):
                        crossed.append((n, group_at(dz, other_y=True)))
        if s + 1 < len(PACE):
            send_halos(crosses, PACE[s], PACE[s + 1])
        windows(s)
        while crossed and (crossed[0][0] < 2 * s - 1 and crossed[0][0] < 6 or s == 5):
            n, group = crossed.pop(0)
            arrived(sv_ref, vy_recv.at[n])
            to_twin(sv_ref, group, 0, 24 + n)
    for which, ref in ((1, sk_ref), (0, sv_ref)):
        half = ref.at[pl.ds(0, NBLK // 2)]
        pltpu.make_async_copy(half, half, core_recv.at[which]).wait()
        if which == 1:
            lax.fori_loop(0, CHUNKS, use_keys, 0)
            whole_weights()
            lax.fori_loop(0, CHUNKS, listed, 0)
    lax.fori_loop(0, CHUNKS, finish, 0)
    for copy in started:
        copy.wait_send()

    def sent(ref, send):
        pltpu.make_async_copy(ref.at[mine], ref.at[mine], send).wait()

    sent(sk_ref, ky_send)
    for n in range(8):
        sent(sv_ref, vy_send.at[n])
    for n in range(32):
        sent(sv_ref, core_send.at[n])
    for ref, send, row, (usual, other) in (
        (sv_ref, vz_send, 0, (4, 5)), (sv_ref, vz_send, 1, (3, 2)), (sk_ref, kz_send, 0, (4, 5)),
        (sk_ref, kz_send, 1, (3, 2)), (sk_ref, kz_send, 2, (3, 4)), (sk_ref, kz_send, 3, (4, 3)),
    ):
        for n in range(max(usual, other)):
            if n < min(usual, other):
                sent(ref, send.at[row, n])
            else:
                pl.when(busy if other > usual else ~busy)(lambda: sent(ref, send.at[row, n]))
    for c in range(CHUNKS):
        for copy in halo(c, 0) + halo(c, 1):
            copy.wait_send()


def shards(queries, keys, values, global_pos, layout):
    bf16 = jnp.bfloat16
    hbm_spec = pl.BlockSpec(memory_space=pltpu.HBM)
    smem_spec = pl.BlockSpec(memory_space=pltpu.SMEM)
    dma = pltpu.SemaphoreType.DMA
    return pl.pallas_call(
        kernel,
        out_shape=jax.ShapeDtypeStruct((ROWS, WIDTH), bf16),
        in_specs=[smem_spec, smem_spec, hbm_spec, hbm_spec, hbm_spec],
        out_specs=pl.BlockSpec(memory_space=pltpu.VMEM),
        scratch_shapes=[
            *[pltpu.VMEM((ROWS, WIDTH), bf16)] * 3,
            *[pltpu.VMEM((BLOCK, WIDTH), bf16)] * 4,
            pltpu.VMEM((SEQS, 4, WIDTH), bf16),
            *[pltpu.VMEM((NBLK, WIDTH), bf16)] * 2,
            *[pltpu.VMEM((ROWS, WIDTH), jnp.float32)] * 4,
            pltpu.VMEM((2 * LINKS, NBLK), bf16),
            pltpu.VMEM((2 * LINKS, WIDTH), bf16),
            pltpu.VMEM((HEADS, ROWS, 2 * LINKS), bf16),
            pltpu.VMEM((2 * HEADS, NBLK), jnp.float32),
            pltpu.VMEM((2, 2 * HEADS, HEAD_DIM), jnp.float32),
            pltpu.VMEM((4, 8, WIDTH), jnp.float32),
            dma((3,)), dma((4, CHUNKS)), dma((4, CHUNKS)), dma((7,)), dma((7,)),
            dma((4, 5)), dma((4, 5)), dma((2, 5)), dma((2, 5)),
            dma, dma, dma((8,)), dma((8,)), dma((32,)), dma((2,)),
        ],
        compiler_params=pltpu.CompilerParams(collective_id=0, has_side_effects=True, vmem_limit_bytes=50 * 1024 * 1024),
    )(global_pos, layout, queries, keys, values)


def solution(mesh):
    rows = P(("grp", "seq"), None)
    in_specs = (rows, rows, rows, P(("grp", "seq")), rows)
    return jax.shard_map(shards, mesh=mesh, in_specs=in_specs, out_specs=rows, check_vma=False)
```
